32 devices in a mesh: section: 2 (over y), row: 4 (over z), col: 4 (over x, core).
Axes of the slice: x: 2, y: 2, z: 4, core: 2. Of those that a mesh axis runs over, the one named last changes fastest.
Arguments:
- tokens: bfloat16 [2, 256, 6144], P(None, 'col', 'row'), may hold values from -6 to 6
- ln_gain: float32 [2, 6144], P('section', 'row'), may hold values from 0.1 to 1.9
- w_query: bfloat16 [2, 6144, 6144], P('section', 'row', 'col'), as said below
- w_key: bfloat16 [2, 6144, 6144], P('section', 'row', 'col'), as said below
- w_value: bfloat16 [2, 6144, 6144], P('section', 'row', 'col'), may hold values from -0.078125 to 0.078125
- w_up: bfloat16 [2, 6144, 24576], P('section', 'row', 'col'), may hold values from -0.078125 to 0.078125
- w_out: bfloat16 [2, 6144, 6144], P('section', 'col', 'row'), may hold values from -0.078125 to 0.078125
- w_down: bfloat16 [2, 24576, 6144], P('section', 'col', 'row'), may hold values from -0.0390625 to 0.0390625
Outputs:
- section_out: bfloat16 [2, 2, 256, 6144], P('section', None, 'col', 'row')
The draws below stay inside these ranges and needn't reach their ends.
Inputs may be any that keep to these rules, and one draw needn't show every extreme that they name: `w_query`: entries are normal with standard deviation 6144 ** -0.5, clipped at six deviations. `w_key`: entries are of the order of 6144 ** -0.5; in some heads the key columns may be up to twenty times larger and correlated with the query columns.
All inputs are finite; a program needn't handle non-finite values.
Results may differ from the reference program's by a relative error of at most 0.02.
Values may be sent and summed in bfloat16 or wider, within the bound.
No kernel may reach another device: no remote copies, remote signals or barrier semaphores. Data moves between devices by JAX's collectives and lax.ppermute only.
A program may use at most 128 MiB of HBM per device.

```python
import jax
import jax.numpy as jnp
from jax import lax

D = 6144
HEADS = 48
MLP = 24576
PATCHES = 256
IMAGES = 2
LAYERS = 2
N_ROW = 4


def base_query(key):
    values = jax.random.normal(jax.random.fold_in(key, 101), (LAYERS, D, D), jnp.float32)
    return jnp.clip(values, -6.0, 6.0) * D ** (-0.5)


def draw_w_query(key, part):
    return base_query(key).astype(jnp.bfloat16)


def draw_w_key(key, part):
    fresh = jax.random.normal(jax.random.fold_in(key, 202), (LAYERS, D, D), jnp.float32)
    fresh = jnp.clip(fresh, -6.0, 6.0) * D ** (-0.5)
    return fresh.astype(jnp.bfloat16)


def level_of(key, dims, split, low, high):
    factor_of, own = 1.0, jax.random.fold_in(key, 6)
    for dim, parts in split:
        heights = jnp.exp(jax.random.uniform(jax.random.fold_in(own, dim), (parts,), jnp.float32, low / len(split), high / len(split)))
        factor_of = factor_of * jnp.repeat(heights, dims[dim] // parts).reshape([-1 if axis == dim else 1 for axis in range(len(dims))])
    return factor_of


def bell_draw(stream_key, extent, spread, reach, cuts=(), dtype=jnp.bfloat16):
    values = spread * jax.random.normal(stream_key, extent, jnp.float32)
    if cuts:
        values = values * level_of(stream_key, extent, cuts, -0.22, 0.18)
    return jnp.clip(values, -reach, reach).astype(dtype)


def setup_inputs(seed: int = 0) -> dict:
    keys = jax.random.split(jax.random.key(seed), 9)
    tokens = bell_draw(keys[0], (IMAGES, PATCHES, D), 1.0, 6.0, ((1, 4), (2, 4)))
    ln_gain = jnp.clip(1.0 + 0.18 * jax.random.normal(keys[1], (LAYERS, D), jnp.float32), 0.1, 1.9)
    w_query = draw_w_query(jax.random.fold_in(keys[8], 71), 0)
    w_key = draw_w_key(jax.random.fold_in(keys[8], 71), 0)
    w_value = bell_draw(keys[4], (LAYERS, D, D), D ** -0.5, 0.078125, ((0, 2), (1, 4), (2, 4)))
    w_up = bell_draw(keys[5], (LAYERS, D, MLP), D ** -0.5, 0.078125, ((0, 2), (1, 4), (2, 4)))
    w_out = bell_draw(keys[6], (LAYERS, D, D), D ** -0.5, 0.078125, ((0, 2), (1, 4), (2, 4)))
    w_down = bell_draw(keys[7], (LAYERS, MLP, D), MLP ** -0.5, 0.0390625, ((0, 2), (1, 4), (2, 4)))
    return dict(tokens=tokens, ln_gain=ln_gain, w_query=w_query, w_key=w_key, w_value=w_value, w_up=w_up, w_out=w_out, w_down=w_down)


EPS = 1e-06

def project(normed, weight):
    block_width = D // N_ROW
    total = jnp.zeros((normed.shape[0], normed.shape[1], weight.shape[1]), jnp.float32)
    for block in range(N_ROW):
        part = jnp.dot(normed[:, :, block * block_width:(block + 1) * block_width], weight[block * block_width:(block + 1) * block_width], preferred_element_type=jnp.float32)
        total = total + lax.optimization_barrier(part.astype(jnp.bfloat16)).astype(jnp.float32)
    return total

def layer(x, gain, wq, wk, wv, wup, wout, wdown):
    xf = x.astype(jnp.float32)
    mean = lax.optimization_barrier(jnp.mean(xf, axis=-1, keepdims=True))
    var = jnp.maximum(lax.optimization_barrier(jnp.mean(xf * xf, axis=-1, keepdims=True)) - mean * mean, 0.0)
    normed = ((xf - mean) * lax.rsqrt(var + EPS) * gain.astype(jnp.float32)).astype(jnp.bfloat16)
    query = project(normed, wq).astype(jnp.bfloat16)
    keyed = project(normed, wk).astype(jnp.bfloat16)
    valued = project(normed, wv).astype(jnp.bfloat16)
    act = jax.nn.gelu(project(normed, wup), approximate=False).astype(jnp.bfloat16)
    head_dim = D // HEADS
    shape = (x.shape[0], x.shape[1], HEADS, head_dim)
    qh = query.reshape(shape).astype(jnp.float32)
    kh = keyed.reshape(shape).astype(jnp.float32)
    vh = valued.reshape(shape).astype(jnp.float32)
    scores = jnp.einsum('bqhd,bkhd->bhqk', qh, kh) / jnp.sqrt(jnp.float32(head_dim))
    scores = scores - lax.optimization_barrier(jnp.max(scores, axis=-1, keepdims=True))
    weights = jnp.exp(scores)
    probs = (weights / lax.optimization_barrier(jnp.sum(weights, axis=-1, keepdims=True))).astype(jnp.bfloat16)
    attn = jnp.einsum('bhqk,bkhd->bqhd', probs.astype(jnp.float32), vh)
    attn = attn.reshape(x.shape).astype(jnp.bfloat16)
    mixed = jnp.dot(attn, wout, preferred_element_type=jnp.float32) + jnp.dot(act, wdown, preferred_element_type=jnp.float32)
    return (xf + mixed).astype(jnp.bfloat16)

def reference(tokens, ln_gain, w_query, w_key, w_value, w_up, w_out, w_down):
    current = tokens
    outputs = []
    for level in range(LAYERS):
        current = layer(current, ln_gain[level], w_query[level], w_key[level], w_value[level], w_up[level], w_out[level], w_down[level])
        outputs.append(current)
    return jnp.stack(outputs)
```

```python
import jax
import jax.numpy as jnp
from jax import lax
from jax.sharding import PartitionSpec as P

D = 6144
HEADS = 48


EPS = 1e-06


def passed_along(value, axis, steps):
    count = lax.axis_size(axis)
    first, last = (max(0, -steps), min(count, count - steps))
    return lax.ppermute(value, axis, [(source, source + steps) for source in range(first, last)])


def pick(which, cases):
    out = cases[-1]
    for number in range(len(cases) - 2, -1, -1):
        out = jnp.where(which == number, cases[number], out)
    return out


def widened(value):
    return value.astype(jnp.float32)


def reduce_to_end(own, direction, distance):
    rows, count = (lax.axis_size("row"), len(own))
    received = []
    for step in range(count + rows - 2):
        chunk = pick(distance, [own[min(max(step - d, 0), count - 1)] for d in range(rows)])
        if received:
            chunk = (widened(chunk) + widened(received[-1])).astype(jnp.bfloat16)
        received.append(passed_along(chunk, "row", direction))
    return received[rows - 2 :]


def spread_from_end(own, direction, distance):
    rows, count = (lax.axis_size("row"), len(own))
    received = []
    for step in range(count + rows - 2):
        chunk = own[min(step, count - 1)]
        if received:
            chunk = jnp.where(distance == 0, chunk, received[-1])
        received.append(passed_along(chunk, "row", direction))
    return [
        pick(distance, [own[j]] + [received[j + d - 1] for d in range(1, rows)])
        for j in range(count)
    ]


def layer(x, weights):
    gain, wq, wk, wv, wup, wout, wdown = weights
    row, rows = (lax.axis_index("row"), lax.axis_size("row"))
    cols = lax.axis_size("col")
    xf = x.astype(jnp.float32)
    sums, squares = lax.psum((jnp.sum(xf, axis=-1), jnp.sum(xf * xf, axis=-1)), "row")
    mean = (sums / D)[..., None]
    var = jnp.maximum((squares / D)[..., None] - mean * mean, 0.0)
    normed = ((xf - mean) * lax.rsqrt(var + EPS) * gain).astype(jnp.bfloat16)
    gathered = lax.all_gather(normed, "col", axis=1, tiled=True)[0]
    half = wq.shape[1] // 2
    pieces = wup.shape[1] // (2 * half)
    low, high = ([], [])
    for weight in (wq, wk, wv):
        part = jnp.dot(gathered, weight, preferred_element_type=jnp.float32).astype(jnp.bfloat16)
        low.append(part[:, :half])
        high.append(part[:, half:])
    part = jnp.dot(gathered, wup, preferred_element_type=jnp.float32).astype(jnp.bfloat16)
    for j in range(pieces):
        low.append(part[:, j * half : (j + 1) * half])
        high.append(part[:, (pieces + j) * half : (pieces + j + 1) * half])
    to_low = reduce_to_end(low, -1, rows - 1 - row)
    to_high = reduce_to_end(high, 1, row)
    first = row == 0
    summed = [
        widened(jnp.where(first, a, b)) + widened(jnp.where(first, p, q))
        for a, b, p, q in zip(low, high, to_low, to_high)
    ]
    head_dim = D // HEADS
    qh, kh, vh = (
        value.astype(jnp.bfloat16).reshape(value.shape[0], half // head_dim, head_dim)
        for value in summed[:3]
    )
    scores = jnp.einsum("qhd,khd->hqk", qh, kh, preferred_element_type=jnp.float32) / jnp.sqrt(
        jnp.float32(head_dim)
    )
    scores = scores - jnp.max(scores, axis=-1, keepdims=True)
    expo = jnp.exp(scores)
    probs = (expo / jnp.sum(expo, axis=-1, keepdims=True)).astype(jnp.bfloat16)
    attn = jnp.einsum("hqk,khd->qhd", probs, vh, preferred_element_type=jnp.float32)
    attn = attn.reshape(gathered.shape[0], half).astype(jnp.bfloat16)
    owned = [attn] + [
        jax.nn.gelu(pre, approximate=False).astype(jnp.bfloat16) for pre in summed[3:]
    ]
    from_low = spread_from_end(owned, 1, row)
    from_high = spread_from_end(owned, -1, rows - 1 - row)
    mixed = jnp.dot(
        jnp.concatenate([from_low[0], from_high[0]], axis=1),
        wout,
        preferred_element_type=jnp.float32,
    )
    for j in range(pieces):
        for base, value in ((j, from_low[1 + j]), (pieces + j, from_high[1 + j])):
            mixed = mixed + jnp.dot(
                value, wdown[base * half : (base + 1) * half], preferred_element_type=jnp.float32
            )
    blocks = mixed.astype(jnp.bfloat16).reshape(cols, mixed.shape[0] // cols, mixed.shape[1])
    blocks = lax.all_to_all(blocks, "col", 0, 0, tiled=True)
    return (xf + jnp.sum(widened(blocks), axis=0)[None]).astype(jnp.bfloat16)


def pass_on(output):
    return passed_along(output, "section", 1)


def local(tokens, ln_gain, w_query, w_key, w_value, w_up, w_out, w_down):
    weights = (ln_gain[0], w_query[0], w_key[0], w_value[0], w_up[0], w_out[0], w_down[0])
    section = lax.axis_index("section")
    sections = lax.axis_size("section")
    result = jnp.zeros_like(tokens)
    images = tokens.shape[0]
    ticks = images + sections - 1
    inbox = jnp.zeros_like(tokens[:1])
    positions = jnp.arange(images, dtype=jnp.int32)
    for tick in range(ticks):
        fresh = tokens[min(tick, images - 1) : min(tick, images - 1) + 1]
        current = jnp.where(section == 0, fresh, inbox)
        output = layer(current, weights)
        slot = tick - section
        result = jnp.where((positions == slot)[:, None, None], output, result)
        if tick + 1 < ticks:
            inbox = pass_on(output)
    return result[None]


def solution(mesh):
    return jax.shard_map(
        local,
        mesh=mesh,
        in_specs=(
            P(None, "col", "row"),
            P("section", "row"),
            P("section", "row", "col"),
            P("section", "row", "col"),
            P("section", "row", "col"),
            P("section", "row", "col"),
            P("section", "col", "row"),
            P("section", "col", "row"),
        ),
        out_specs=P("section", None, "col", "row"),
        check_vma=False,
    )
```
